512 devices in a mesh: elem: 128 (over z, y, core), gpt: 4 (over x).
Axes of the slice: x: 4, y: 8, z: 8, core: 2. Of those that a mesh axis runs over, the one named last changes fastest.
Arguments:
- slab_kelvin: float32 [16, 65536], P(None, 'elem'), may hold values from 190 to 310
- moisture_mass_load: float32 [16, 65536], P(None, 'elem'), may hold values from 0.1 to 1
- dioxide_mass_load: float32 [16, 65536], P(None, 'elem'), may hold values from 0.2 to 1
- slab_depth_share: float32 [16, 65536], P(None, 'elem'), may hold values from 0.01 to 0.06
- lower_node_slot: int32 [16, 65536], P(None, 'elem'), may hold values from 0 to 57
- upper_node_share: float32 [16, 65536], P(None, 'elem'), may hold values from 0 to 1
- ground_skin_kelvin: float32 [65536], P('elem'), may hold values from 230 to 310
- ground_reflectivity: float32 [65536], P('elem'), may hold values from 0.05 to 0.8
- sun_angle_class: int32 [65536], P('elem'), may hold values from 0 to 127, as said below
- owner_profile_routes: int32 [65536], P('elem'), may hold values from 0 to 511, as said below
- sunlit_angle_factors: float32 [64], replicated, may hold values from 0.05 to 1
- thermal_absorptivity: bfloat16 [128, 118], P('gpt'), may hold values from 0.0019989014 to 2
- sunlight_absorptivity: bfloat16 [112, 118], P('gpt'), may hold values from 0.0019989014 to 1
- emission_quadrature_share: float32 [128], P('gpt'), may hold values from 0.00390625 to 0.015625
- insolation_quadrature_share: float32 [112], P('gpt'), may hold values from 0.004464286 to 0.017857144
Outputs:
- heat_lw: float32 [16, 65536], P('gpt', 'elem')
- heat_sw: float32 [16, 65536], P('gpt', 'elem')
- surface_flux: float32 [4, 65536], P('gpt', 'elem')
The draws below stay inside these ranges and needn't reach their ends.
Inputs may be any that keep to these rules, and one draw needn't show every extreme that they name: `sun_angle_class`: A column is sunlit when its bin is below 64. Every span receives exactly 256 sunlit columns, and an owner gives equally many sunlit columns to every span. `owner_profile_routes`: for each owner, a permutation of its local column numbers 0 to 511.
All inputs are finite; a program needn't handle non-finite values.
Results may differ from the reference program's by a relative error of at most 0.0014.
Values may be sent and summed in bfloat16 or wider, within the bound.
A program may use at most 64 MiB of HBM per device.

```python
import math
import jax
import jax.numpy as jnp
from jax import lax

G_LW = 128
G_SW = 112
NP = 59
SLAB_AMOUNT = 16
DAY_BINS = 64
COL_DEV = 512
PEER = 4
ALL_PROFILES = 65536
N_ELEM = 128


def sky_layout(key):
    base = jax.random.fold_in(key, 11)
    keys = jax.random.split(base, 5)
    per_peer = COL_DEV // N_ELEM
    owners = jnp.arange(N_ELEM, dtype=jnp.int32)
    turn = jax.random.randint(keys[0], (), 0, N_ELEM)
    split_at = jax.random.randint(keys[1], (), 0, per_peer + 1)
    place = (owners + turn) % N_ELEM
    middle = N_ELEM // 2
    sunny_share = jnp.where(place < middle - 1, per_peer, jnp.where(place == middle - 1, split_at, jnp.where(place == middle, per_peer - split_at, 0)))
    shuffled = jax.vmap(lambda sub_key: jax.random.permutation(sub_key, COL_DEV))(jax.random.split(keys[2], N_ELEM)).astype(jnp.int32)
    ranks = jnp.argsort(shuffled, axis=1)
    sunny_total = sunny_share * N_ELEM
    sunlit = ranks < sunny_total[:, None]
    spans = jnp.arange(N_ELEM, dtype=jnp.int32)[None, :, None]
    slots = jnp.arange(per_peer, dtype=jnp.int32)[None, None, :]
    share = sunny_share[:, None, None]
    pick = jnp.where(slots < share, spans * share + slots, sunny_total[:, None, None] + spans * (per_peer - share) + slots - share)
    base_order = jnp.take_along_axis(shuffled, pick.reshape(N_ELEM, COL_DEV), axis=1).reshape(N_ELEM, N_ELEM, per_peer)
    scores = jax.random.randint(keys[3], (N_ELEM, N_ELEM, per_peer), 0, 1 << 20) * per_peer + slots
    within = jnp.argsort(scores, axis=2)
    pack = jnp.take_along_axis(base_order, within, axis=2).reshape(-1).astype(jnp.int32)
    bins = jax.random.randint(keys[4], (N_ELEM, COL_DEV), 0, DAY_BINS) + jnp.where(sunlit, 0, DAY_BINS)
    return (bins.reshape(-1).astype(jnp.int32), pack)


def draw_sun_angle_class(key, part):
    return sky_layout(key)[0]


def draw_owner_profile_routes(key, part):
    return sky_layout(key)[1]


def with_ends(values, own_key, least, largest):
    extent = values.shape
    spot = [jax.random.randint(jax.random.fold_in(own_key, axis), (), 0, extent[axis]) for axis in range(len(extent))]
    values = values.at[tuple(spot)].set(least)
    longest = extent.index(max(extent))
    spot[longest] = (spot[longest] + 1) % extent[longest]
    return values.at[tuple(spot)].set(largest)


def levels(stream_key, dims, cuts, smallest, largest):
    factor_of = 1.0
    for axis_at, shards_of in cuts:
        steps = jax.random.uniform(jax.random.fold_in(jax.random.fold_in(stream_key, 6), axis_at), (shards_of,), jnp.float32, smallest / len(cuts), largest / len(cuts))
        factor_of = factor_of * jnp.repeat(jnp.exp(steps), dims[axis_at] // shards_of).reshape((-1,) + (1,) * (len(dims) - 1 - axis_at))
    return factor_of


def setup_inputs(seed: int = 0) -> dict:
    key_list = jax.random.split(jax.random.key(seed), 16)
    return {
        "slab_kelvin": jnp.clip(190.0 + 120.0 * jax.random.uniform(key_list[0], (SLAB_AMOUNT, ALL_PROFILES), jnp.float32) ** levels(key_list[0], (SLAB_AMOUNT, ALL_PROFILES), ((1, 128),), -0.2, 0.2), 190.0, 310.0),
        "moisture_mass_load": jnp.clip(jnp.exp(math.log(1.0) - 2.3025851 * jax.random.uniform(key_list[1], (SLAB_AMOUNT, ALL_PROFILES), jnp.float32) ** levels(key_list[1], (SLAB_AMOUNT, ALL_PROFILES), ((1, 128),), -0.2, 0.2)), 0.1, 1.0),
        "dioxide_mass_load": jnp.clip(jnp.exp(math.log(1.0) - 1.609438 * jax.random.uniform(key_list[2], (SLAB_AMOUNT, ALL_PROFILES), jnp.float32) ** levels(key_list[2], (SLAB_AMOUNT, ALL_PROFILES), ((1, 128),), -0.2, 0.2)), 0.2, 1.0),
        "slab_depth_share": jnp.clip(jnp.exp(math.log(0.06) - 1.7917595 * jax.random.uniform(key_list[3], (SLAB_AMOUNT, ALL_PROFILES), jnp.float32) ** levels(key_list[3], (SLAB_AMOUNT, ALL_PROFILES), ((1, 128),), -0.2, 0.2)), 0.01, 0.06),
        "lower_node_slot": with_ends(jax.random.randint(key_list[4], (SLAB_AMOUNT, ALL_PROFILES), 0, NP - 1), jax.random.fold_in(key_list[4], 1), 0, (NP - 1) - 1).astype(jnp.int32),
        "upper_node_share": jnp.clip(1.0 * jax.random.uniform(key_list[5], (SLAB_AMOUNT, ALL_PROFILES), jnp.float32) ** levels(key_list[5], (SLAB_AMOUNT, ALL_PROFILES), ((1, 128),), -0.2, 0.2), 0.0, 1.0),
        "ground_skin_kelvin": jnp.clip(230.0 + 80.0 * jax.random.uniform(key_list[6], (ALL_PROFILES,), jnp.float32) ** levels(key_list[6], (ALL_PROFILES,), ((0, 128),), -0.2, 0.2), 230.0, 310.0),
        "ground_reflectivity": jnp.clip(0.05 + 0.75 * jax.random.uniform(key_list[7], (ALL_PROFILES,), jnp.float32) ** levels(key_list[7], (ALL_PROFILES,), ((0, 128),), -0.2, 0.2), 0.05, 0.8),
        "sun_angle_class": draw_sun_angle_class(jax.random.fold_in(key_list[15], 71), 0),
        "owner_profile_routes": draw_owner_profile_routes(jax.random.fold_in(key_list[15], 71), 0),
        "sunlit_angle_factors": jnp.clip(jnp.exp(jax.random.uniform(key_list[10], (DAY_BINS,), jnp.float32, math.log(0.05), math.log(1.0))), 0.05, 1.0),
        "thermal_absorptivity": jnp.clip(jnp.exp(math.log(2.0) - 6.9083047 * jax.random.uniform(key_list[11], (G_LW, 2 * NP), jnp.float32) ** levels(key_list[11], (G_LW, 2 * NP), ((0, 4),), -0.2, 0.2)), 0.0019989014, 2.0).astype(jnp.bfloat16),
        "sunlight_absorptivity": jnp.clip(jnp.exp(math.log(1.0) - 6.2151576 * jax.random.uniform(key_list[12], (G_SW, 2 * NP), jnp.float32) ** levels(key_list[12], (G_SW, 2 * NP), ((0, 4),), -0.2, 0.2)), 0.0019989014, 1.0).astype(jnp.bfloat16),
        "emission_quadrature_share": jnp.clip(jnp.exp(math.log(0.015625) - 1.3862944 * jax.random.uniform(key_list[13], (G_LW,), jnp.float32) ** levels(key_list[13], (G_LW,), ((0, 4),), -0.2, 0.2)), 0.00390625, 0.015625),
        "insolation_quadrature_share": jnp.clip(jnp.exp(math.log(0.017857144) - 1.3862944 * jax.random.uniform(key_list[14], (G_SW,), jnp.float32) ** levels(key_list[14], (G_SW,), ((0, 4),), -0.2, 0.2)), 0.004464286, 0.017857144),
    }


def compose(earlier, later):
    return earlier[0] * later[0], later[0] * earlier[1] + later[1]


def zenith_cosine(bins, table):
    node_index = jnp.arange(table.shape[0], dtype=jnp.int32)[:, None]
    return jnp.sum(jnp.where(bins[None, :] == node_index, table[:, None], 0.0), axis=0)


def absorber(state_inputs, node_count):
    node_values = jnp.arange(node_count).astype(state_inputs.dtype)[:, None, None]
    node_index = state_inputs[4][None]
    weight = state_inputs[5][None]
    interp_weights = jnp.where(node_values == node_index, 1.0 - weight, 0.0) + jnp.where(node_values == node_index + 1.0, weight, 0.0)
    amount = jnp.concatenate([interp_weights * state_inputs[1][None], interp_weights * state_inputs[2][None]], axis=0).astype(jnp.bfloat16)
    return amount.reshape(2 * node_count, -1)


def longwave(tau, state_inputs, profile, planck):
    transmit = jnp.exp(-1.66 * tau)
    source = planck[:, None, None] * (state_inputs[0][None] / 250.0) ** 4
    emitted = source * (1.0 - transmit)
    downward = lax.associative_scan(compose, (transmit, emitted), axis=1)[1]
    rise_gain, rise_add = lax.associative_scan(compose, (transmit, emitted), axis=1, reverse=True)
    ground = planck[:, None] * (profile[0][None] / 250.0) ** 4
    up_top = rise_gain * ground[:, None, :] + rise_add
    up_bottom = jnp.concatenate([up_top[:, 1:], ground[:, None, :]], axis=1)
    down_top = jnp.concatenate([jnp.zeros_like(downward[:, :1]), downward[:, :-1]], axis=1)
    heating = jnp.sum((up_bottom - downward) - (up_top - down_top), axis=0) / state_inputs[3]
    return heating, jnp.sum(downward[:, -1], axis=0), jnp.sum(up_top[:, 0], axis=0)


def shortwave(tau, state_inputs, profile, solar):
    sun_height_factor = profile[2]
    safe_cosine = jnp.where(sun_height_factor > 0.0, sun_height_factor, 1.0)
    incident = solar[:, None] * sun_height_factor[None]
    direct_bottom = incident[:, None, :] * jnp.exp(-jnp.cumsum(tau / safe_cosine[None, None, :], axis=1))
    direct_top = jnp.concatenate([incident[:, None, :], direct_bottom[:, :-1]], axis=1)
    depth_below = jnp.flip(jnp.cumsum(jnp.flip(1.66 * tau, 1), axis=1), 1)
    ground = profile[1][None] * direct_bottom[:, -1]
    up_top = ground[:, None, :] * jnp.exp(-depth_below)
    up_bottom = jnp.concatenate([up_top[:, 1:], ground[:, None, :]], axis=1)
    heating = jnp.sum((direct_top - up_top) - (direct_bottom - up_bottom), axis=0) / state_inputs[3]
    return heating, jnp.sum(direct_bottom[:, -1], axis=0), jnp.sum(up_top[:, 0], axis=0)


def radiate(state_inputs, profile, thermal_absorptivity, sunlight_absorptivity, planck, solar):
    node_count = thermal_absorptivity.shape[1] // 2
    slab_heights = state_inputs.shape[1]
    profile_ordinal = state_inputs.shape[2]
    amount = absorber(state_inputs, node_count)
    tau_long = jnp.dot(thermal_absorptivity, amount, preferred_element_type=jnp.float32).reshape(thermal_absorptivity.shape[0], slab_heights, profile_ordinal)
    heat_long, down_ground, outgoing = longwave(tau_long, state_inputs, profile, planck)
    tau_short = jnp.dot(sunlight_absorptivity, amount, preferred_element_type=jnp.float32).reshape(sunlight_absorptivity.shape[0], slab_heights, profile_ordinal)
    heat_short, direct_ground, reflected = shortwave(tau_short, state_inputs, profile, solar)
    return jnp.stack([heat_long, heat_short], axis=1), jnp.stack([down_ground, outgoing, direct_ground, reflected], axis=0)


def reference(slab_kelvin, moisture_mass_load, dioxide_mass_load, slab_depth_share, lower_node_slot, upper_node_share, ground_skin_kelvin, ground_reflectivity, sun_angle_class, owner_profile_routes, sunlit_angle_factors, thermal_absorptivity, sunlight_absorptivity, emission_quadrature_share, insolation_quadrature_share):
    sun_height_factor = zenith_cosine(sun_angle_class, sunlit_angle_factors)
    state_inputs = jnp.stack([slab_kelvin, moisture_mass_load, dioxide_mass_load, slab_depth_share, lower_node_slot.astype(jnp.float32), upper_node_share])
    profile = jnp.stack([ground_skin_kelvin, ground_reflectivity, sun_height_factor])

    def one_block(block_start):
        field_part = lax.dynamic_slice_in_dim(state_inputs, block_start, COL_DEV, 2)
        side_part = lax.dynamic_slice_in_dim(profile, block_start, COL_DEV, 1)
        return radiate(field_part, side_part, thermal_absorptivity, sunlight_absorptivity, emission_quadrature_share, insolation_quadrature_share)

    heating, fluxes = lax.map(one_block, jnp.arange(N_ELEM, dtype=jnp.int32) * COL_DEV)
    heating = jnp.moveaxis(heating, 0, 2).reshape(SLAB_AMOUNT, 2, ALL_PROFILES)
    fluxes = jnp.moveaxis(fluxes, 0, 1).reshape(4, ALL_PROFILES)
    pack_grid = owner_profile_routes.reshape(N_ELEM, N_ELEM, PEER)
    global_cols = pack_grid + (jnp.arange(N_ELEM, dtype=jnp.int32) * COL_DEV)[:, None, None]
    span_cols = jnp.transpose(global_cols, (1, 0, 2)).reshape(-1).astype(jnp.int32)
    return heating[:, 0], heating[:, 1], fluxes[:, span_cols]
```

```python
import jax
import jax.numpy as jnp
from jax import lax
from jax.experimental import pallas as pl
from jax.experimental.pallas import tpu as pltpu
from jax.sharding import PartitionSpec as P

MESH = pl.DeviceIdType.MESH
LOG2E = 1.4426950408889634
DIFFUSE = -1.66 * LOG2E
LAYERS = 16
COLS = 512
LANES = 128
WIDE = 256
NODES = 59
GL = 32
GS = 28
GPT = 4
NZ = 8
NW = 16
STACK = 10


def by_lane(row, index):
    return jnp.take_along_axis(row, index, axis=1, mode="promise_in_bounds")


def as_column(row, length):
    r = lax.broadcasted_iota(jnp.int32, (length, length), 0)
    c = lax.broadcasted_iota(jnp.int32, (length, length), 1)
    return jnp.sum(jnp.where(r == c, jnp.broadcast_to(row, (length, length)), 0.0), axis=1, keepdims=True)


def kernel(
    kelvin, moisture, dioxide, depth, slot, share, skin, albedo, bins, routes, table,
    thermal, sunlight, planck, solar,
    heat_lw, heat_sw, flux_out,
    coef, rows, cosine, trans, emit, down_sum, direct_sum, up_sum, reflect_sum, flux, heat, heat_in,
    part, part_in, mine, z_in, w_out, w_in,
    heat_send, heat_recv, part_send, part_recv, z_send, z_recv, w_send, w_recv,
):
    e = lax.axis_index("elem")
    q = lax.axis_index("gpt")
    z = e // NW
    w = e % NW
    barrier = pltpu.get_barrier_semaphore()

    def gpt_peer(i):
        return {"elem": e, "gpt": (q + i) % GPT}

    def z_peer(i):
        return {"elem": ((z + i) % NZ) * NW + w, "gpt": q}

    def w_peer(i):
        return {"elem": z * NW + (w + i) % NW, "gpt": q}

    for i in range(1, GPT):
        pl.semaphore_signal(barrier, inc=1, device_id=gpt_peer(i), device_id_type=MESH)
    for i in range(1, NZ):
        pl.semaphore_signal(barrier, inc=1, device_id=z_peer(i), device_id_type=MESH)
    for i in range(1, NW):
        pl.semaphore_signal(barrier, inc=1, device_id=w_peer(i), device_id_type=MESH)

    coef[...] = jnp.zeros_like(coef)
    coef[0:GL, 0 : 2 * NODES] = thermal[...]
    coef[GL : GL + GS, 0 : 2 * NODES] = sunlight[...]
    rows[...] = lax.broadcasted_iota(jnp.int32, (LANES, WIDE), 0).astype(jnp.float32).astype(jnp.bfloat16)
    p_col = as_column(planck[...], GL)
    s_col = as_column(solar[...], GS)
    s_col = jnp.concatenate([s_col, jnp.zeros((GL - GS, 1), jnp.float32)], axis=0)

    factors = jnp.concatenate([table[...], table[...]], axis=1)
    factors = jnp.broadcast_to(factors, (8, LANES))
    for k in range(COLS // LANES):
        b = bins[:, k * LANES : (k + 1) * LANES]
        picked = by_lane(factors, jnp.broadcast_to(b & 63, (8, LANES)))[0:1]
        cosine[:, k * LANES : (k + 1) * LANES] = jnp.where(b < 64, picked, 0.0)

    a = coef[...]
    for half in range(COLS // WIDE):
        cols = pl.ds(half * WIDE, WIDE)
        cos = cosine[:, cols]
        slant = -LOG2E / jnp.where(cos > 0.0, cos, 1.0)

        def down_step(l, carry):
            down, direct = carry
            at = pl.ds(l, 1)
            upper = share[at, cols]
            lower = 1.0 - upper
            m = moisture[at, cols]
            d = dioxide[at, cols]
            node = slot[at, cols].astype(jnp.float32)
            bf = jnp.bfloat16
            n0 = node.astype(bf)
            n1 = (node + 1.0).astype(bf)
            n2 = (node + NODES).astype(bf)
            n3 = (node + (NODES + 1)).astype(bf)
            m0 = (lower * m).astype(bf)
            m1 = (upper * m).astype(bf)
            d0 = (lower * d).astype(bf)
            d1 = (upper * d).astype(bf)
            zero = jnp.zeros((), bf)
            r = rows[0:48, :]
            top = jnp.where(r == n0, m0, jnp.where(r == n1, m1, zero))
            r = rows[48:64, :]
            mid = jnp.where(r == n0, m0, jnp.where(r == n1, m1, jnp.where(r == n2, d0, jnp.where(r == n3, d1, zero))))
            r = rows[64:128, :]
            low = jnp.where(r == n2, d0, jnp.where(r == n3, d1, zero))
            amount = jnp.concatenate([top, mid, low], axis=0)
            tau = jnp.dot(a, amount, preferred_element_type=jnp.float32)
            tau_lw = tau[0:GL]
            tau_sw = tau[GL : 2 * GL]
            x = kelvin[at, cols] * (1.0 / 250.0)
            x = x * x
            warm = x * x
            t = jnp.exp2(tau_lw * DIFFUSE)
            source = (p_col * warm) * (1.0 - t)
            down = t * down + source
            trans[l, 0:GL, :] = t
            emit[l] = source
            down_sum[at, cols] = jnp.sum(down, axis=0, keepdims=True)
            trans[l, GL : 2 * GL, :] = jnp.exp2(tau_sw * DIFFUSE)
            direct = direct * jnp.exp2(tau_sw * slant)
            direct_sum[at, cols] = jnp.sum(direct, axis=0, keepdims=True)
            return down, direct

        incident = s_col * cos
        down, direct = lax.fori_loop(0, LAYERS, down_step, (jnp.zeros((GL, WIDE), jnp.float32), incident))

        x = skin[:, cols] * (1.0 / 250.0)
        x = x * x
        up = p_col * (x * x)
        reflected = albedo[:, cols] * direct

        def up_step(k, carry):
            up, reflected = carry
            l = LAYERS - 1 - k
            up = trans[l, 0:GL, :] * up + emit[l]
            up_sum[pl.ds(l, 1), cols] = jnp.sum(up, axis=0, keepdims=True)
            reflected = reflected * trans[l, GL : 2 * GL, :]
            reflect_sum[pl.ds(l, 1), cols] = jnp.sum(reflected, axis=0, keepdims=True)
            return up, reflected

        up_sum[LAYERS : LAYERS + 1, cols] = jnp.sum(up, axis=0, keepdims=True)
        reflect_sum[LAYERS : LAYERS + 1, cols] = jnp.sum(reflected, axis=0, keepdims=True)
        up, reflected = lax.fori_loop(0, LAYERS, up_step, (up, reflected))
        first = jnp.sum(incident, axis=0, keepdims=True)
        flux[0:1, cols] = down_sum[LAYERS - 1 : LAYERS, cols]
        flux[1:2, cols] = up_sum[0:1, cols]
        flux[2:3, cols] = direct_sum[LAYERS - 1 : LAYERS, cols]
        flux[3:4, cols] = reflect_sum[0:1, cols]
        for l in range(LAYERS):
            inverse = 1.0 / depth[l : l + 1, cols]
            low_net = up_sum[l + 1 : l + 2, cols] - down_sum[l : l + 1, cols]
            if l:
                top_net = up_sum[l : l + 1, cols] - down_sum[l - 1 : l, cols]
                top_sun = direct_sum[l - 1 : l, cols] - reflect_sum[l : l + 1, cols]
            else:
                top_net = up_sum[0:1, cols]
                top_sun = first - reflect_sum[0:1, cols]
            low_sun = direct_sum[l : l + 1, cols] - reflect_sum[l + 1 : l + 2, cols]
            heat[l // 4, l % 4 : l % 4 + 1, cols] = (low_net - top_net) * inverse
            heat[l // 4, 4 + l % 4 : 5 + l % 4, cols] = (top_sun - low_sun) * inverse

    order = routes[...]
    for k in range(COLS // LANES):
        index = jnp.broadcast_to(order[:, k * LANES : (k + 1) * LANES], (8, LANES))
        within = index & (LANES - 1)
        block = index >> 7
        picked = jnp.zeros((8, LANES), jnp.float32)
        for s in range(COLS // LANES):
            picked = jnp.where(block == s, by_lane(flux[:, s * LANES : (s + 1) * LANES], within), picked)
        for r in range(4):
            part[r, k : k + 1, :] = picked[r : r + 1]

    pl.semaphore_wait(barrier, (GPT - 1) + (NZ - 1) + (NW - 1))

    part_copies = []
    for i in range(1, GPT):
        c = pltpu.make_async_remote_copy(
            src_ref=part.at[(q + i) % GPT], dst_ref=part_in.at[i - 1],
            send_sem=part_send.at[i - 1], recv_sem=part_recv.at[i - 1],
            device_id=gpt_peer(i), device_id_type=MESH,
        )
        c.start()
        part_copies.append(c)
    heat_copies = []
    for i in range(1, GPT):
        c = pltpu.make_async_remote_copy(
            src_ref=heat.at[(q + i) % GPT], dst_ref=heat_in.at[i - 1],
            send_sem=heat_send.at[i - 1], recv_sem=heat_recv.at[i - 1],
            device_id=gpt_peer(i), device_id_type=MESH,
        )
        c.start()
        heat_copies.append(c)
    for c in part_copies:
        c.wait_recv()
    whole = part[q] + part_in[0] + part_in[1] + part_in[2]
    for k in range(4):
        mine[k] = whole[k : k + 1]

    z_copies = []
    for i in range(1, NZ):
        to = (z + i) % NZ
        c = pltpu.make_async_remote_copy(
            src_ref=mine.at[to // 2], dst_ref=z_in.at[z],
            send_sem=z_send.at[i - 1], recv_sem=z_recv.at[i - 1],
            device_id=z_peer(i), device_id_type=MESH,
        )
        c.start()
        z_copies.append(c)
    z_in[z] = mine[z // 2]

    for c in heat_copies:
        c.wait_recv()
    owned = heat[q] + heat_in[0] + heat_in[1] + heat_in[2]
    heat_lw[...] = owned[0:4]
    heat_sw[...] = owned[4:8]

    for c in z_copies:
        c.wait_recv()
    half_start = 16 * (z % 2)
    lane = lax.broadcasted_iota(jnp.int32, (NW, LANES), 1) >> 2
    line = lax.broadcasted_iota(jnp.int32, (NW, LANES), 0)
    source = (lane + (32 - half_start) - line) & 31
    out = jnp.zeros((NW, LANES), jnp.float32)
    for s in range(NZ):
        row = z_in[s]
        if s:
            row = pltpu.roll(row, 4 * s, 1)
        out = jnp.where(source == s, jnp.broadcast_to(row, (NW, LANES)), out)
    for k in range(NW):
        w_out[k] = out[k : k + 1]

    w_copies = []
    for i in range(1, NW):
        c = pltpu.make_async_remote_copy(
            src_ref=w_out.at[(w + i) % NW], dst_ref=w_in.at[w],
            send_sem=w_send.at[i - 1], recv_sem=w_recv.at[i - 1],
            device_id=w_peer(i), device_id_type=MESH,
        )
        c.start()
        w_copies.append(c)
    w_in[w] = w_out[w]
    for c in w_copies:
        c.wait_recv()
    start = half_start + w
    lane = lax.broadcasted_iota(jnp.int32, (NZ, LANES), 1) >> 2
    line = lax.broadcasted_iota(jnp.int32, (NZ, LANES), 0)
    source = (lane + (32 - start) - line) & 31
    out = jnp.zeros((NZ, LANES), jnp.float32)
    for s in range(NW):
        row = w_in[s]
        if s:
            row = pltpu.roll(row, 4 * s, 1)
        out = jnp.where(source == s, jnp.broadcast_to(row, (NZ, LANES)), out)
    out = pltpu.roll(out, (LANES - 4 * start) % LANES, 1)
    first_half = lax.broadcasted_iota(jnp.int32, (1, LANES), 1) < 64
    for k in range(4):
        even = pltpu.roll(out, (LANES - 8 * k) % LANES, 1) if k else out
        odd = pltpu.roll(out, (LANES - 4 * (2 * k + 1) + 64) % LANES, 1)
        flux_out[:, k * LANES : (k + 1) * LANES] = jnp.where(
            first_half, even[2 * k : 2 * k + 1], odd[2 * k + 1 : 2 * k + 2]
        )

    for c in part_copies + heat_copies + z_copies + w_copies:
        c.wait_send()


def local(
    slab_kelvin, moisture_mass_load, dioxide_mass_load, slab_depth_share, lower_node_slot, upper_node_share,
    ground_skin_kelvin, ground_reflectivity, sun_angle_class, owner_profile_routes, sunlit_angle_factors,
    thermal_absorptivity, sunlight_absorptivity, emission_quadrature_share, insolation_quadrature_share,
):
    f32 = jnp.float32
    vmem = pl.BlockSpec(memory_space=pltpu.VMEM)
    dma = pltpu.SemaphoreType.DMA
    return pl.pallas_call(
        kernel,
        out_shape=(
            jax.ShapeDtypeStruct((LAYERS // GPT, COLS), f32),
            jax.ShapeDtypeStruct((LAYERS // GPT, COLS), f32),
            jax.ShapeDtypeStruct((1, COLS), f32),
        ),
        in_specs=[vmem] * 15,
        out_specs=(vmem, vmem, vmem),
        scratch_shapes=[
            pltpu.VMEM((2 * GL, LANES), jnp.bfloat16),
            pltpu.VMEM((LANES, WIDE), jnp.bfloat16),
            pltpu.VMEM((1, COLS), f32),
            pltpu.VMEM((LAYERS, 2 * GL, WIDE), f32),
            pltpu.VMEM((LAYERS, GL, WIDE), f32),
            pltpu.VMEM((LAYERS, COLS), f32),
            pltpu.VMEM((LAYERS, COLS), f32),
            pltpu.VMEM((24, COLS), f32),
            pltpu.VMEM((24, COLS), f32),
            pltpu.VMEM((8, COLS), f32),
            pltpu.VMEM((GPT, 8, COLS), f32),
            pltpu.VMEM((GPT - 1, 8, COLS), f32),
            pltpu.VMEM((GPT, 4, LANES), f32),
            pltpu.VMEM((GPT - 1, 4, LANES), f32),
            pltpu.VMEM((4, 1, LANES), f32),
            pltpu.VMEM((NZ, 1, LANES), f32),
            pltpu.VMEM((NW, 1, LANES), f32),
            pltpu.VMEM((NW, 1, LANES), f32),
            dma((GPT - 1,)), dma((GPT - 1,)), dma((GPT - 1,)), dma((GPT - 1,)),
            dma((NZ - 1,)), dma((NZ - 1,)), dma((NW - 1,)), dma((NW - 1,)),
        ],
        compiler_params=pltpu.CompilerParams(collective_id=0, has_side_effects=True),
    )(
        slab_kelvin, moisture_mass_load, dioxide_mass_load, slab_depth_share, lower_node_slot, upper_node_share,
        ground_skin_kelvin.reshape(1, COLS), ground_reflectivity.reshape(1, COLS),
        sun_angle_class.reshape(1, COLS), owner_profile_routes.reshape(1, COLS),
        sunlit_angle_factors.reshape(1, 64), thermal_absorptivity, sunlight_absorptivity,
        emission_quadrature_share.reshape(1, GL), insolation_quadrature_share.reshape(1, GS),
    )


def solution(mesh):
    e = P("elem")
    eg = P(None, "elem")
    in_specs = (eg,) * 6 + (e,) * 4 + (P(), P("gpt", None), P("gpt", None), P("gpt"), P("gpt"))
    out_specs = (P("gpt", "elem"), P("gpt", "elem"), P("gpt", "elem"))
    return jax.shard_map(local, mesh=mesh, in_specs=in_specs, out_specs=out_specs, check_vma=False)
```

```python
import jax
import jax.numpy as jnp
from jax import lax
from jax.experimental import pallas as pl
from jax.experimental.pallas import tpu as pltpu
from jax.sharding import PartitionSpec as P

MESH = pl.DeviceIdType.MESH
LOG2E = 1.4426950408889634
DIFFUSE = -1.66 * LOG2E
LAYERS = 16
COLS = 512
LANES = 128
WIDE = 256
NODES = 59
GL = 32
GS = 28
GPT = 4
NZ = 8
NW = 16
UNROLL = 4
HEAT_UNROLL = 2
F32 = jnp.float32
BF16 = jnp.bfloat16

ZQ_STEPS = sorted(
    [(dz, dq) for dz in range(NZ) for dq in range(GPT) if dz or dq],
    key=lambda s: -(min(s[0], NZ - s[0]) + min(s[1], GPT - s[1])),
)
W_STEPS = sorted(range(1, NW), key=lambda s: -min(s, NW - s))


def by_lane(row, index):
    return jnp.take_along_axis(row, index, axis=1, mode="promise_in_bounds")


def as_column(row, length):
    r = lax.broadcasted_iota(jnp.int32, (length, length), 0)
    c = lax.broadcasted_iota(jnp.int32, (length, length), 1)
    return jnp.sum(jnp.where(r == c, jnp.broadcast_to(row, (length, length)), 0.0), axis=1, keepdims=True)


def total(x):
    return jnp.sum(x, axis=0, keepdims=True)


def fourth(x):
    x = x * (1.0 / 250.0)
    x = x * x
    return x * x


def kernel(*refs):
    args, refs = refs[:15], refs[15:]
    heat_lw, heat_sw, flux_out = refs[:3]
    local, refs = refs[3:18], refs[18:]
    (
        kelvin, moisture, dioxide, depth, slot, share, skin, albedo, bins, routes, table,
        thermal, sunlight, planck, solar,
    ) = local
    (
        coef, rows, cosine, node, m0, m1, d0, d1, warm, trans, emit, tau_sun,
        down_sum, direct_sum, up_sum, reflect_sum, net, sun, flux, heat, heat_in,
        part, zq_in, w_out, w_in,
        load_sem, heat_send, heat_recv, zq_send, zq_recv, w_send, w_recv,
    ) = refs
    e = lax.axis_index("elem")
    q = lax.axis_index("gpt")
    z = e // NW
    w = e % NW
    barrier = pltpu.get_barrier_semaphore()

    loads = [pltpu.make_async_copy(args[i], local[i], load_sem.at[i]) for i in range(15)]
    for c in loads:
        c.start()

    def zq_peer(dz, dq):
        return {"elem": ((z + dz) % NZ) * NW + w, "gpt": (q + dq) % GPT}

    def w_peer(dw):
        return {"elem": z * NW + (w + dw) % NW, "gpt": q}

    for dz, dq in ZQ_STEPS:
        pl.semaphore_signal(barrier, inc=1, device_id=zq_peer(dz, dq), device_id_type=MESH)
    for dw in W_STEPS:
        pl.semaphore_signal(barrier, inc=1, device_id=w_peer(dw), device_id_type=MESH)

    coef[...] = jnp.zeros_like(coef)
    rows[...] = lax.broadcasted_iota(jnp.int32, (LANES, WIDE), 0).astype(F32).astype(BF16)
    down_sum[0:1, :] = jnp.zeros((1, COLS), F32)
    for c in loads:
        c.wait()
    coef[0:GL, 0 : 2 * NODES] = thermal[...]
    coef[GL : GL + GS, 0 : 2 * NODES] = sunlight[...]
    p_col = as_column(planck[...], GL)
    s_col = as_column(solar[...], GS)
    s_col = jnp.concatenate([s_col, jnp.zeros((GL - GS, 1), F32)], axis=0)

    upper = share[...]
    lower = 1.0 - upper
    m = moisture[...]
    d = dioxide[...]
    m0[...] = lower * m
    m1[...] = upper * m
    d0[...] = lower * d
    d1[...] = upper * d
    node[...] = slot[...].astype(F32)
    warm[...] = fourth(kelvin[...])
    factors = jnp.concatenate([table[...], table[...]], axis=1)
    factors = jnp.broadcast_to(factors, (8, LANES))
    for k in range(COLS // LANES):
        b = bins[:, k * LANES : (k + 1) * LANES]
        picked = by_lane(factors, jnp.broadcast_to(b & 63, (8, LANES)))[0:1]
        cosine[:, k * LANES : (k + 1) * LANES] = jnp.where(b < 64, picked, 0.0)

    a = coef[...]

    def spread(ref, l, cols):
        return jnp.broadcast_to(ref[pl.ds(l, 1), cols], (16, WIDE)).astype(BF16)

    def slanted(cols):
        cos = cosine[:, cols]
        return -LOG2E / jnp.where(cos > 0.0, cos, 1.0)

    for half in range(COLS // WIDE):
        cols = pl.ds(half * WIDE, WIDE)

        def flux_layer(l, carry):
            down, clear, up, depth_sun = carry
            n0 = spread(node, l, cols)
            n1 = n0 + jnp.asarray(1, BF16)
            n2 = n0 + jnp.asarray(NODES, BF16)
            n3 = n0 + jnp.asarray(NODES + 1, BF16)
            w0, w1 = spread(m0, l, cols), spread(m1, l, cols)
            c0, c1 = spread(d0, l, cols), spread(d1, l, cols)
            zero = jnp.zeros((16, WIDE), BF16)
            blocks = []
            for k in range(8):
                r = rows[16 * k : 16 * k + 16, :]
                x = zero
                if k >= 3:
                    x = jnp.where(r == n2, c0, jnp.where(r == n3, c1, x))
                if k <= 3:
                    x = jnp.where(r == n0, w0, jnp.where(r == n1, w1, x))
                blocks.append(x)
            tau = jnp.dot(a, jnp.concatenate(blocks, axis=0), preferred_element_type=F32)
            t = jnp.exp2(tau[0:GL] * DIFFUSE)
            source = (p_col * warm[pl.ds(l, 1), cols]) * (1.0 - t)
            trans[l, :, cols] = t
            emit[l, :, cols] = source
            tau_sun[l, :, cols] = tau[GL : 2 * GL]
            up = up + clear * source
            clear = clear * t
            down = t * down + source
            return down, clear, up, depth_sun + tau[GL : 2 * GL]

        def flux_step(i, carry):
            for k in range(UNROLL):
                carry = flux_layer(i * UNROLL + k, carry)
            return carry

        blank = jnp.zeros((GL, WIDE), F32)
        carry = (blank, jnp.ones((GL, WIDE), F32), blank, blank)
        down, clear, up, depth_sun = lax.fori_loop(0, LAYERS // UNROLL, flux_step, carry)
        direct = (s_col * cosine[:, cols]) * jnp.exp2(depth_sun * slanted(cols))
        flux[0:1, cols] = total(down)
        flux[1:2, cols] = total(up + clear * (p_col * fourth(skin[:, cols])))
        flux[2:3, cols] = total(direct)
        flux[3:4, cols] = total((albedo[:, cols] * direct) * jnp.exp2(depth_sun * DIFFUSE))

    order = routes[...]
    for k in range(COLS // LANES):
        index = jnp.broadcast_to(order[:, k * LANES : (k + 1) * LANES], (8, LANES))
        within = index & (LANES - 1)
        block = index >> 7
        picked = jnp.zeros((8, LANES), F32)
        for s in range(COLS // LANES):
            picked = jnp.where(block == s, by_lane(flux[:, s * LANES : (s + 1) * LANES], within), picked)
        for r in range(GPT):
            part[r, k] = picked[r : r + 1]

    pl.semaphore_wait(barrier, len(ZQ_STEPS) + len(W_STEPS))

    zq_copies = []
    for i, (dz, dq) in enumerate(ZQ_STEPS):
        c = pltpu.make_async_remote_copy(
            src_ref=part.at[(q + dq) % GPT, ((z + dz) % NZ) // 2], dst_ref=zq_in.at[q, z],
            send_sem=zq_send.at[i], recv_sem=zq_recv.at[i],
            device_id=zq_peer(dz, dq), device_id_type=MESH,
        )
        c.start()
        zq_copies.append(c)
    zq_in[q, z] = part[q, z // 2]

    for half in range(COLS // WIDE):
        cols = pl.ds(half * WIDE, WIDE)
        slant = slanted(cols)
        incident = s_col * cosine[:, cols]
        depth_sun = tau_sun[0, :, cols]
        for l in range(1, LAYERS):
            depth_sun = depth_sun + tau_sun[l, :, cols]
        ground = albedo[:, cols] * (incident * jnp.exp2(depth_sun * slant))
        skin_up = p_col * fourth(skin[:, cols])

        def heat_layer(l, carry):
            down, up, direct, reflected = carry
            k = LAYERS - 1 - l
            down = trans[l, :, cols] * down + emit[l, :, cols]
            down_sum[pl.ds(l + 1, 1), cols] = total(down)
            up = trans[k, :, cols] * up + emit[k, :, cols]
            up_sum[pl.ds(k, 1), cols] = total(up)
            direct = direct * jnp.exp2(tau_sun[l, :, cols] * slant)
            direct_sum[pl.ds(l + 1, 1), cols] = total(direct)
            reflected = reflected * jnp.exp2(tau_sun[k, :, cols] * DIFFUSE)
            reflect_sum[pl.ds(k, 1), cols] = total(reflected)
            return down, up, direct, reflected

        def heat_step(i, carry):
            for k in range(HEAT_UNROLL):
                carry = heat_layer(i * HEAT_UNROLL + k, carry)
            return carry

        up_sum[LAYERS : LAYERS + 1, cols] = total(skin_up)
        direct_sum[0:1, cols] = total(incident)
        reflect_sum[LAYERS : LAYERS + 1, cols] = total(ground)
        carry = (jnp.zeros((GL, WIDE), F32), skin_up, incident, ground)
        lax.fori_loop(0, LAYERS // HEAT_UNROLL, heat_step, carry)

    top = slice(0, LAYERS)
    low = slice(1, LAYERS + 1)
    faces = slice(0, LAYERS + 1)
    net[faces, :] = up_sum[faces, :] - down_sum[faces, :]
    sun[faces, :] = direct_sum[faces, :] - reflect_sum[faces, :]
    inverse = 1.0 / depth[...]
    lw = (net[low, :] - net[top, :]) * inverse
    sw = (sun[top, :] - sun[low, :]) * inverse
    for r in range(GPT):
        heat[r, 0:4, :] = lw[4 * r : 4 * r + 4]
        heat[r, 4:8, :] = sw[4 * r : 4 * r + 4]

    heat_copies = []
    for i in range(1, GPT):
        c = pltpu.make_async_remote_copy(
            src_ref=heat.at[(q + i) % GPT], dst_ref=heat_in.at[i - 1],
            send_sem=heat_send.at[i - 1], recv_sem=heat_recv.at[i - 1],
            device_id=zq_peer(0, i), device_id_type=MESH,
        )
        c.start()
        heat_copies.append(c)

    for c in zq_copies:
        c.wait_recv()
    half_start = 16 * (z % 2)
    lane = lax.broadcasted_iota(jnp.int32, (NW, LANES), 1) >> 2
    line = lax.broadcasted_iota(jnp.int32, (NW, LANES), 0)
    source = (lane + (32 - half_start) - line) & 31
    out = jnp.zeros((NW, LANES), F32)
    for s in range(NZ):
        row = (zq_in[0, s] + zq_in[1, s]) + (zq_in[2, s] + zq_in[3, s])
        if s:
            row = pltpu.roll(row, 4 * s, 1)
        out = jnp.where(source == s, jnp.broadcast_to(row, (NW, LANES)), out)
    for k in range(NW):
        w_out[k] = out[k : k + 1]

    w_copies = []
    for i, dw in enumerate(W_STEPS):
        c = pltpu.make_async_remote_copy(
            src_ref=w_out.at[(w + dw) % NW], dst_ref=w_in.at[w],
            send_sem=w_send.at[i], recv_sem=w_recv.at[i],
            device_id=w_peer(dw), device_id_type=MESH,
        )
        c.start()
        w_copies.append(c)
    w_in[w] = w_out[w]

    for c in heat_copies:
        c.wait_recv()
    owned = (heat[q] + heat_in[0]) + (heat_in[1] + heat_in[2])
    heat_lw[...] = owned[0:4]
    heat_sw[...] = owned[4:8]

    for c in w_copies:
        c.wait_recv()
    start = half_start + w
    lane = lax.broadcasted_iota(jnp.int32, (NZ, LANES), 1) >> 2
    line = lax.broadcasted_iota(jnp.int32, (NZ, LANES), 0)
    source = (lane + (32 - start) - line) & 31
    out = jnp.zeros((NZ, LANES), F32)
    for s in range(NW):
        row = w_in[s]
        if s:
            row = pltpu.roll(row, 4 * s, 1)
        out = jnp.where(source == s, jnp.broadcast_to(row, (NZ, LANES)), out)
    out = pltpu.roll(out, (LANES - 4 * start) % LANES, 1)
    first_half = lax.broadcasted_iota(jnp.int32, (1, LANES), 1) < 64
    for k in range(4):
        even = pltpu.roll(out, (LANES - 8 * k) % LANES, 1) if k else out
        odd = pltpu.roll(out, (LANES - 4 * (2 * k + 1) + 64) % LANES, 1)
        flux_out[:, k * LANES : (k + 1) * LANES] = jnp.where(
            first_half, even[2 * k : 2 * k + 1], odd[2 * k + 1 : 2 * k + 2]
        )

    for c in zq_copies + heat_copies + w_copies:
        c.wait_send()


def hand_out(*refs):
    for source, target in zip(refs[:3], refs[3:]):
        target[...] = source[...]


def local(
    slab_kelvin, moisture_mass_load, dioxide_mass_load, slab_depth_share, lower_node_slot, upper_node_share,
    ground_skin_kelvin, ground_reflectivity, sun_angle_class, owner_profile_routes, sunlit_angle_factors,
    thermal_absorptivity, sunlight_absorptivity, emission_quadrature_share, insolation_quadrature_share,
):
    dma = pltpu.SemaphoreType.DMA
    vmem = pl.BlockSpec(memory_space=pltpu.VMEM)
    args = (
        slab_kelvin, moisture_mass_load, dioxide_mass_load, slab_depth_share, lower_node_slot, upper_node_share,
        ground_skin_kelvin.reshape(1, COLS), ground_reflectivity.reshape(1, COLS),
        sun_angle_class.reshape(1, COLS), owner_profile_routes.reshape(1, COLS),
        sunlit_angle_factors.reshape(1, 64), thermal_absorptivity, sunlight_absorptivity,
        emission_quadrature_share.reshape(1, GL), insolation_quadrature_share.reshape(1, GS),
    )
    state = (LAYERS, COLS)
    faces = (24, COLS)
    results = ((LAYERS // GPT, COLS), (LAYERS // GPT, COLS), (1, COLS))
    held = pl.pallas_call(
        kernel,
        out_shape=tuple(pltpu.VMEM(s, F32) for s in results),
        in_specs=[pl.BlockSpec(memory_space=pl.ANY)] * 15,
        out_specs=(vmem, vmem, vmem),
        scratch_shapes=[pltpu.VMEM(x.shape, x.dtype) for x in args]
        + [
            pltpu.VMEM((2 * GL, LANES), BF16),
            pltpu.VMEM((LANES, WIDE), BF16),
            pltpu.VMEM((1, COLS), F32),
        ]
        + [pltpu.VMEM(state, F32)] * 6
        + [pltpu.VMEM((LAYERS, GL, COLS), F32)] * 3
        + [pltpu.VMEM(faces, F32)] * 6
        + [
            pltpu.VMEM((8, COLS), F32),
            pltpu.VMEM((GPT, 8, COLS), F32),
            pltpu.VMEM((GPT - 1, 8, COLS), F32),
            pltpu.VMEM((GPT, 4, 1, LANES), F32),
            pltpu.VMEM((GPT, NZ, 1, LANES), F32),
            pltpu.VMEM((NW, 1, LANES), F32),
            pltpu.VMEM((NW, 1, LANES), F32),
            dma((15,)), dma((GPT - 1,)), dma((GPT - 1,)),
            dma((len(ZQ_STEPS),)), dma((len(ZQ_STEPS),)), dma((len(W_STEPS),)), dma((len(W_STEPS),)),
        ],
        compiler_params=pltpu.CompilerParams(collective_id=0, has_side_effects=True),
    )(*args)
    return pl.pallas_call(
        hand_out,
        out_shape=tuple(jax.ShapeDtypeStruct(s, F32) for s in results),
        in_specs=[vmem] * 3,
        out_specs=(vmem, vmem, vmem),
    )(*(pltpu.with_memory_space_constraint(h, pltpu.VMEM) for h in held))


def solution(mesh):
    e = P("elem")
    eg = P(None, "elem")
    in_specs = (eg,) * 6 + (e,) * 4 + (P(), P("gpt", None), P("gpt", None), P("gpt"), P("gpt"))
    out_specs = (P("gpt", "elem"), P("gpt", "elem"), P("gpt", "elem"))
    return jax.shard_map(local, mesh=mesh, in_specs=in_specs, out_specs=out_specs, check_vma=False)
```
